32 devices in a mesh: rep: 2 (over x), fsdp: 16 (over z, y, core).
Axes of the slice: x: 2, y: 2, z: 4, core: 2. Of those that a mesh axis runs over, the one named last changes fastest.
Arguments:
- tokens: bfloat16 [256, 3584], P(('rep', 'fsdp')), may hold values from -6 to 6
- targets: bfloat16 [256, 3584], P(('rep', 'fsdp')), may hold values from -6 to 6
- gate_weight: bfloat16 [3584, 18944], P(None, 'fsdp'), may hold values from -0.09375 to 0.09375
- up_weight: bfloat16 [3584, 18944], P(None, 'fsdp'), may hold values from -0.09375 to 0.09375
- down_weight: bfloat16 [18944, 3584], P('fsdp'), may hold values from -0.046875 to 0.046875
- gate_direction: bfloat16 [3584, 18944], P(None, 'fsdp'), may hold values from -0.09375 to 0.09375
- up_direction: bfloat16 [3584, 18944], P(None, 'fsdp'), may hold values from -0.09375 to 0.09375
- down_direction: bfloat16 [18944, 3584], P('fsdp'), may hold values from -0.046875 to 0.046875
Outputs:
- hvp_gate: float32 [3584, 18944], P(None, 'fsdp')
- hvp_up: float32 [3584, 18944], P(None, 'fsdp')
- hvp_down: float32 [18944, 3584], P('fsdp')
The draws below stay inside these ranges and needn't reach their ends.
All inputs are finite; a program needn't handle non-finite values.
Results may differ from the reference program's by a relative error of at most 0.0069.
Values may be sent and summed in bfloat16 or wider, within the bound.
A program may use at most 192 MiB of HBM per device.

```python
import jax
import jax.numpy as jnp
from jax import lax

D = 3584
FF = 18944
TOKENS = 256


def block_scale(key, extent, pieces, least, top_value):
    def one(position, shards_of):
        steps = jax.random.uniform(jax.random.fold_in(jax.random.fold_in(key, 6), position), (shards_of,), jnp.float32, least / len(pieces), top_value / len(pieces))
        return jnp.repeat(jnp.exp(steps), extent[position] // shards_of).reshape((-1,) + (1,) * (len(extent) - position - 1))

    level = one(*pieces[0])
    for cut in pieces[1:]:
        level = level * one(*cut)
    return level


def bell_draw(own_key, shape, spread, limit, shards=(), kind=jnp.bfloat16):
    factor_of = block_scale(own_key, shape, shards, -0.22, 0.18) if shards else 1.0
    entries = jax.random.normal(own_key, shape, jnp.float32) * spread * factor_of
    return jnp.minimum(jnp.maximum(entries, -limit), limit).astype(kind)


def setup_inputs(seed: int = 0) -> dict:
    streams_of = jax.random.split(jax.random.key(seed), 9)
    return {
        "tokens": bell_draw(streams_of[0], (TOKENS, D), 1.0, 6.0, ((0, 32),)),
        "targets": bell_draw(streams_of[1], (TOKENS, D), 1.0, 6.0, ((0, 32),)),
        "gate_weight": bell_draw(streams_of[2], (D, FF), D ** -0.5, 0.09375, ((1, 16),)),
        "up_weight": bell_draw(streams_of[3], (D, FF), D ** -0.5, 0.09375, ((1, 16),)),
        "down_weight": bell_draw(streams_of[4], (FF, D), FF ** -0.5, 0.046875, ((0, 16),)),
        "gate_direction": bell_draw(streams_of[5], (D, FF), D ** -0.5, 0.09375, ((1, 16),)),
        "up_direction": bell_draw(streams_of[6], (D, FF), D ** -0.5, 0.09375, ((1, 16),)),
        "down_direction": bell_draw(streams_of[7], (FF, D), FF ** -0.5, 0.046875, ((0, 16),)),
    }


def silu_parts(gate):
    sigmoid_value = jax.nn.sigmoid(gate)
    slope = sigmoid_value * (1.0 + gate * (1.0 - sigmoid_value))
    bend = sigmoid_value * (1.0 - sigmoid_value) * (2.0 + gate * (1.0 - 2.0 * sigmoid_value))
    return gate * sigmoid_value, slope, bend


def inner_rows(left, right):
    return lax.dot_general(left, right, (((0,), (0,)), ((), ())), preferred_element_type=jnp.float32)


def reference(tokens, targets, gate_weight, up_weight, down_weight, gate_direction, up_direction, down_direction):
    gate = jnp.dot(tokens, gate_weight, preferred_element_type=jnp.float32)
    up = jnp.dot(tokens, up_weight, preferred_element_type=jnp.float32)
    gate_tangent = jnp.dot(tokens, gate_direction, preferred_element_type=jnp.float32)
    up_tangent = jnp.dot(tokens, up_direction, preferred_element_type=jnp.float32)
    activation, slope, bend = silu_parts(gate)
    hidden = (activation * up).astype(jnp.bfloat16)
    hidden_tangent = (slope * gate_tangent * up + activation * up_tangent).astype(jnp.bfloat16)
    output = jnp.dot(hidden, down_weight, preferred_element_type=jnp.float32)
    output_tangent = jnp.dot(hidden_tangent, down_weight, preferred_element_type=jnp.float32) + jnp.dot(hidden, down_direction, preferred_element_type=jnp.float32)
    error = (output - targets.astype(jnp.float32)).astype(jnp.bfloat16)
    error_tangent = output_tangent.astype(jnp.bfloat16)
    back = jnp.dot(error, down_weight.T, preferred_element_type=jnp.float32)
    back_tangent = jnp.dot(error_tangent, down_weight.T, preferred_element_type=jnp.float32) + jnp.dot(error, down_direction.T, preferred_element_type=jnp.float32)
    gate_grad_tangent = (back_tangent * up * slope + back * up_tangent * slope + back * up * bend * gate_tangent).astype(jnp.bfloat16)
    up_grad_tangent = (back_tangent * activation + back * slope * gate_tangent).astype(jnp.bfloat16)
    hvp_gate = inner_rows(tokens, gate_grad_tangent)
    hvp_up = inner_rows(tokens, up_grad_tangent)
    hvp_down = inner_rows(hidden_tangent, error) + inner_rows(hidden, error_tangent)
    return hvp_gate, hvp_up, hvp_down
```

```python
import functools

import jax
import jax.numpy as jnp
from jax import lax
from jax.experimental import pallas as pl
from jax.experimental.pallas import tpu as pltpu
from jax.sharding import PartitionSpec as P

MESH = pl.DeviceIdType.MESH
F32 = jnp.float32
BF16 = jnp.bfloat16


def silu_parts(gate):
    sigmoid_value = jax.nn.sigmoid(gate)
    slope = sigmoid_value * (1.0 + gate * (1.0 - sigmoid_value))
    bend = sigmoid_value * (1.0 - sigmoid_value) * (2.0 + gate * (1.0 - 2.0 * sigmoid_value))
    return (gate * sigmoid_value, slope, bend)


def inner_rows(left, right):
    return lax.dot_general(left, right, (((0,), (0,)), ((), ())), preferred_element_type=F32)


class Place:
    def __init__(self, reps, bits):
        me = lax.axis_index("fsdp")
        rep = lax.axis_index("rep")
        self.reps, self.bits = reps, bits
        self.bit = [lax.rem(me // (1 << s), 2) for s in range(bits)]
        self.partner = [me + (1 << s) * (1 - 2 * self.bit[s]) for s in range(bits)]
        self.other_rep = [lax.rem(rep + d, reps) for d in range(1, reps)]
        self.slot = sum(self.bit[s] * (1 << (bits - 1 - s)) for s in range(bits))

    def meet(self):
        barrier = pltpu.get_barrier_semaphore()
        for partner in self.partner:
            pl.semaphore_signal(
                barrier, inc=1, device_id={"fsdp": partner}, device_id_type=MESH
            )
        for rep in self.other_rep:
            pl.semaphore_signal(barrier, inc=1, device_id={"rep": rep}, device_id_type=MESH)
        pl.semaphore_wait(barrier, self.bits + self.reps - 1)

    def base(self, k):
        return self.slot // (1 << k) * (1 << k)

    def partner_base(self, k):
        return self.base(k) + (1 << k) * (1 - 2 * self.bit[self.bits - 1 - k])


class Gather:
    def __init__(self, place, out, fs, fr, xs, xr, ws, wr):
        self.place, self.out = place, out
        self.fs, self.fr, self.xs, self.xr, self.ws, self.wr = fs, fr, xs, xr, ws, wr
        self.sent = []

    def _send(self, src, dst, send, recv, device):
        copy = pltpu.make_async_remote_copy(
            src_ref=src, dst_ref=dst, send_sem=send, recv_sem=recv,
            device_id=device, device_id_type=MESH,
        )
        copy.start()
        self.sent.append(copy)

    def across(self, piece, src, first, count):
        reps = self.place.reps
        for d in range(1, reps):
            self._send(
                src, self.out.at[reps - d, pl.ds(first, count)],
                self.xs.at[d - 1, piece], self.xr.at[reps - d - 1, piece],
                {"rep": self.place.other_rep[d - 1]},
            )

    def stage(self, k, src=None):
        place = self.place
        window = self.out.at[0, pl.ds(place.base(k), 1 << k)]
        self._send(
            window if src is None else src, window, self.fs.at[k], self.fr.at[k],
            {"fsdp": place.partner[place.bits - 1 - k]},
        )

    def start(self, src):
        self.stage(0, src)
        self.across(0, src, self.place.slot, 1)

    def arrive(self, k):
        window = self.out.at[0, pl.ds(self.place.partner_base(k), 1 << k)]
        pltpu.make_async_copy(window, window, self.fr.at[k]).wait()

    def forward(self, k):
        place = self.place
        self.arrive(k)
        if k + 1 < place.bits:
            self.stage(k + 1)
            first = place.partner_base(k)
            self.across(k + 1, self.out.at[0, pl.ds(first, 1 << k)], first, 1 << k)

    def pieces(self):
        yield 0, self.place.slot, 1
        for k in range(self.place.bits - 1):
            yield k + 1, self.place.partner_base(k), 1 << k

    def relay(self, piece, first, count):
        for d in range(1, self.place.reps):
            window = self.out.at[d, pl.ds(first, count)]
            pltpu.make_async_copy(window, window, self.xr.at[d - 1, piece]).wait()
            self._send(
                window, window, self.ws.at[d - 1, piece], self.wr.at[d - 1, piece],
                {"fsdp": self.place.partner[0]},
            )

    def finish(self):
        place = self.place
        for piece, first, count in self.pieces():
            far = first + place.partner_base(place.bits - 1) - place.base(place.bits - 1)
            for d in range(1, place.reps):
                window = self.out.at[d, pl.ds(far, count)]
                pltpu.make_async_copy(window, window, self.wr.at[d - 1, piece]).wait()
        for copy in self.sent:
            copy.wait_send()


def gather_semaphores(reps, bits):
    dma = pltpu.SemaphoreType.DMA
    others = max(reps - 1, 1)
    return [dma((bits,)), dma((bits,))] + [dma((others, bits))] * 4


def tokens_kernel(reps, bits, tokens_ref, out_ref, local, *sems):
    place = Place(reps, bits)
    own = pltpu.make_async_copy(tokens_ref, out_ref.at[0, pl.ds(place.slot, 1)], local)
    own.start()
    place.meet()
    gather = Gather(place, out_ref, *sems)
    gather.start(tokens_ref)
    own.wait()
    for k in range(bits - 1):
        gather.forward(k)
    for piece in gather.pieces():
        gather.relay(*piece)
    gather.arrive(bits - 1)
    gather.finish()


def errors_kernel(reps, bits, *refs):
    primal_ref, tangent_ref, targets_ref, error_ref, error_tangent_ref = refs[:5]
    refs = refs[5:]
    parts = (primal_ref, tangent_ref)
    outs = (error_ref, error_tangent_ref)
    landing = [refs[c * bits : (c + 1) * bits] for c in range(2)]
    refs = refs[2 * bits :]
    totals = [refs[c * bits : (c + 1) * bits] for c in range(2)]
    refs = refs[2 * bits :]
    send, recv, local = refs[:3]
    sems = [refs[3:9], refs[9:15]]

    place = Place(reps, bits)
    place.meet()
    copies = {}

    def begin(c, j, src):
        half = 1 << (bits - 1 - j)
        copies[c, j] = pltpu.make_async_remote_copy(
            src_ref=src.at[pl.ds((1 - place.bit[j]) * half, half)],
            dst_ref=landing[c][j],
            send_sem=send.at[c, j],
            recv_sem=recv.at[c, j],
            device_id={"fsdp": place.partner[j]},
            device_id_type=MESH,
        )
        copies[c, j].start()

    current = list(parts)
    for c in range(2):
        begin(c, 0, current[c])
    gathers = [Gather(place, outs[c], *sems[c]) for c in range(2)]
    own = []
    for j in range(bits):
        half = 1 << (bits - 1 - j)
        for c in range(2):
            copies[c, j].wait_recv()
            keep = place.bit[j] * half
            source, came, total = current[c], landing[c][j], totals[c][j]
            if j < bits - 1:

                def add(i, carry, source=source, came=came, total=total, keep=keep):
                    total[i] = (source[keep + i].astype(F32) + came[i].astype(F32)).astype(BF16)
                    return carry

                lax.fori_loop(0, half, add, 0)
                current[c] = total
                begin(c, j + 1, total)
            else:
                whole = source[keep].astype(F32) + came[0].astype(F32)
                if c == 0:
                    whole = whole - targets_ref[0].astype(F32)
                total[0] = whole.astype(BF16)
                gathers[c].start(total)
                own.append(
                    pltpu.make_async_copy(
                        total, outs[c].at[0, pl.ds(place.slot, 1)], local.at[c]
                    )
                )
                own[c].start()
    for c in range(2):
        own[c].wait()
    for k in range(bits - 1):
        for c in range(2):
            gathers[c].forward(k)
    for k, piece in enumerate(gathers[0].pieces()):
        for c in range(2):
            gathers[c].relay(*piece)
    for c in range(2):
        gathers[c].arrive(bits - 1)
        gathers[c].finish()
    for copy in copies.values():
        copy.wait_send()


def vmem(count):
    return [pl.BlockSpec(memory_space=pltpu.VMEM)] * count


def gather_tokens(tokens, reps, bits):
    rows, width = tokens.shape
    fsdp = 1 << bits
    out = pl.pallas_call(
        functools.partial(tokens_kernel, reps, bits),
        out_shape=jax.ShapeDtypeStruct((reps, fsdp, rows, width), BF16),
        in_specs=vmem(1),
        out_specs=vmem(1)[0],
        scratch_shapes=[pltpu.SemaphoreType.DMA] + gather_semaphores(reps, bits),
        compiler_params=pltpu.CompilerParams(collective_id=0, has_side_effects=True),
        cost_estimate=pl.CostEstimate(flops=0, bytes_accessed=60_000_000, transcendentals=0),
        name="tokens_gather",
    )(tokens.reshape(1, rows, width))
    return out.reshape(reps * fsdp * rows, width)


def exchange_errors(primal, tangent, targets, reps, bits):
    rows, width = targets.shape
    fsdp = 1 << bits
    dma = pltpu.SemaphoreType.DMA
    halves = [pltpu.VMEM((1 << (bits - 1 - j), rows, width), BF16) for j in range(bits)]
    shape = jax.ShapeDtypeStruct((reps, fsdp, rows, width), BF16)
    error, error_tangent = pl.pallas_call(
        functools.partial(errors_kernel, reps, bits),
        out_shape=(shape, shape),
        in_specs=vmem(3),
        out_specs=tuple(vmem(2)),
        scratch_shapes=halves * 4
        + [dma((2, bits)), dma((2, bits)), dma((2,))]
        + gather_semaphores(reps, bits) * 2,
        compiler_params=pltpu.CompilerParams(
            collective_id=1, has_side_effects=True, vmem_limit_bytes=56 * 1024 * 1024
        ),
        cost_estimate=pl.CostEstimate(flops=0, bytes_accessed=120_000_000, transcendentals=0),
        name="errors_exchange",
    )(
        primal.reshape(fsdp, rows, width),
        tangent.reshape(fsdp, rows, width),
        targets.reshape(1, rows, width),
    )
    total = reps * fsdp * rows
    return error.reshape(total, width), error_tangent.reshape(total, width)


def on_device(
    reps,
    bits,
    tokens,
    targets,
    gate_weight,
    up_weight,
    down_weight,
    gate_direction,
    up_direction,
    down_direction,
):
    gathered = gather_tokens(tokens, reps, bits)
    mine = gathered.shape[0] // reps
    gate = jnp.dot(gathered, gate_weight, preferred_element_type=F32)
    up = jnp.dot(gathered, up_weight, preferred_element_type=F32)
    gate_tangent = jnp.dot(gathered, gate_direction, preferred_element_type=F32)
    up_tangent = jnp.dot(gathered, up_direction, preferred_element_type=F32)
    activation, slope, bend = silu_parts(gate)
    hidden = (activation * up).astype(BF16)
    hidden_tangent = (slope * gate_tangent * up + activation * up_tangent).astype(BF16)
    primal = jnp.dot(hidden[:mine], down_weight, preferred_element_type=F32).astype(BF16)
    tangent = (
        jnp.dot(hidden_tangent[:mine], down_weight, preferred_element_type=F32)
        + jnp.dot(hidden[:mine], down_direction, preferred_element_type=F32)
    ).astype(BF16)
    error, error_tangent = exchange_errors(primal, tangent, targets, reps, bits)
    back = jnp.dot(error, down_weight.T, preferred_element_type=F32)
    back_tangent = jnp.dot(error_tangent, down_weight.T, preferred_element_type=F32) + jnp.dot(
        error, down_direction.T, preferred_element_type=F32
    )
    gate_grad_tangent = (
        back_tangent * up * slope + back * up_tangent * slope + back * up * bend * gate_tangent
    ).astype(BF16)
    up_grad_tangent = (back_tangent * activation + back * slope * gate_tangent).astype(BF16)
    hvp_gate = inner_rows(gathered, gate_grad_tangent)
    hvp_up = inner_rows(gathered, up_grad_tangent)
    hvp_down = inner_rows(
        jnp.concatenate([hidden_tangent, hidden], axis=0),
        jnp.concatenate([error, error_tangent], axis=0),
    )
    return (hvp_gate, hvp_up, hvp_down)


def solution(mesh):
    reps = mesh.shape["rep"]
    bits = mesh.shape["fsdp"].bit_length() - 1
    in_specs = (
        P(("rep", "fsdp"), None),
        P(("rep", "fsdp"), None),
        P(None, "fsdp"),
        P(None, "fsdp"),
        P("fsdp", None),
        P(None, "fsdp"),
        P(None, "fsdp"),
        P("fsdp", None),
    )
    out_specs = (P(None, "fsdp"), P(None, "fsdp"), P("fsdp", None))
    return jax.shard_map(
        functools.partial(on_device, reps, bits),
        mesh=mesh, in_specs=in_specs, out_specs=out_specs, check_vma=False,
    )
```

```python
import functools

import jax
import jax.numpy as jnp
from jax import lax
from jax.experimental import pallas as pl
from jax.experimental.pallas import tpu as pltpu
from jax.sharding import PartitionSpec as P

MESH = pl.DeviceIdType.MESH
SPLIT = 2
F32 = jnp.float32
BF16 = jnp.bfloat16


def silu_parts(gate):
    sigmoid_value = jax.nn.sigmoid(gate)
    slope = sigmoid_value * (1.0 + gate * (1.0 - sigmoid_value))
    bend = sigmoid_value * (1.0 - sigmoid_value) * (2.0 + gate * (1.0 - 2.0 * sigmoid_value))
    return (gate * sigmoid_value, slope, bend)


def inner_rows(left, right):
    return lax.dot_general(left, right, (((0,), (0,)), ((), ())), preferred_element_type=F32)


class Place:
    def __init__(self, reps, bits):
        me = lax.axis_index("fsdp")
        rep = lax.axis_index("rep")
        self.reps, self.bits = reps, bits
        self.bit = [lax.rem(me // (1 << s), 2) for s in range(bits)]
        self.partner = [me + (1 << s) * (1 - 2 * self.bit[s]) for s in range(bits)]
        self.other_rep = [lax.rem(rep + d, reps) for d in range(1, reps)]
        self.slot = sum(self.bit[s] * (1 << (bits - 1 - s)) for s in range(bits))

    def meet(self):
        barrier = pltpu.get_barrier_semaphore()
        for partner in self.partner:
            pl.semaphore_signal(
                barrier, inc=1, device_id={"fsdp": partner}, device_id_type=MESH
            )
        for rep in self.other_rep:
            pl.semaphore_signal(barrier, inc=1, device_id={"rep": rep}, device_id_type=MESH)
        pl.semaphore_wait(barrier, self.bits + self.reps - 1)

    def base(self, k):
        return self.slot // (1 << k) * (1 << k)

    def partner_base(self, k):
        return self.base(k) + (1 << k) * (1 - 2 * self.bit[self.bits - 1 - k])


class Gather:
    def __init__(self, place, out, fs, fr, xs, xr, ws, wr):
        self.place, self.out = place, out
        self.fs, self.fr, self.xs, self.xr, self.ws, self.wr = fs, fr, xs, xr, ws, wr
        self.sent = []

    def _send(self, src, dst, send, recv, device):
        copy = pltpu.make_async_remote_copy(
            src_ref=src, dst_ref=dst, send_sem=send, recv_sem=recv,
            device_id=device, device_id_type=MESH,
        )
        copy.start()
        self.sent.append(copy)

    def across(self, piece, src, first, count):
        reps = self.place.reps
        for d in range(1, reps):
            self._send(
                src, self.out.at[reps - d, pl.ds(first, count)],
                self.xs.at[d - 1, piece], self.xr.at[reps - d - 1, piece],
                {"rep": self.place.other_rep[d - 1]},
            )

    def stage(self, k, src=None):
        place = self.place
        window = self.out.at[0, pl.ds(place.base(k), 1 << k)]
        self._send(
            window if src is None else src, window, self.fs.at[k], self.fr.at[k],
            {"fsdp": place.partner[place.bits - 1 - k]},
        )

    def start(self, src):
        self.stage(0, src)
        self.across(0, src, self.place.slot, 1)

    def arrive(self, k):
        window = self.out.at[0, pl.ds(self.place.partner_base(k), 1 << k)]
        pltpu.make_async_copy(window, window, self.fr.at[k]).wait()

    def forward(self, k):
        place = self.place
        self.arrive(k)
        if k + 1 < place.bits:
            self.stage(k + 1)
            first = place.partner_base(k)
            self.across(k + 1, self.out.at[0, pl.ds(first, 1 << k)], first, 1 << k)

    def pieces(self):
        yield 0, self.place.slot, 1
        for k in range(self.place.bits - 1):
            yield k + 1, self.place.partner_base(k), 1 << k

    def relay(self, piece, first, count):
        for d in range(1, self.place.reps):
            window = self.out.at[d, pl.ds(first, count)]
            pltpu.make_async_copy(window, window, self.xr.at[d - 1, piece]).wait()
            self._send(
                window, window, self.ws.at[d - 1, piece], self.wr.at[d - 1, piece],
                {"fsdp": self.place.partner[0]},
            )

    def finish(self):
        place = self.place
        for piece, first, count in self.pieces():
            far = first + place.partner_base(place.bits - 1) - place.base(place.bits - 1)
            for d in range(1, place.reps):
                window = self.out.at[d, pl.ds(far, count)]
                pltpu.make_async_copy(window, window, self.wr.at[d - 1, piece]).wait()
        for copy in self.sent:
            copy.wait_send()


def gather_semaphores(reps, bits):
    dma = pltpu.SemaphoreType.DMA
    others = max(reps - 1, 1)
    return [dma((bits,)), dma((bits,))] + [dma((others, bits))] * 4


def tokens_kernel(reps, bits, tokens_ref, out_ref, local, *sems):
    place = Place(reps, bits)
    own = pltpu.make_async_copy(tokens_ref, out_ref.at[0, pl.ds(place.slot, 1)], local)
    own.start()
    place.meet()
    gather = Gather(place, out_ref, *sems)
    gather.start(tokens_ref)
    own.wait()
    for k in range(bits - 1):
        gather.forward(k)
    for piece in gather.pieces():
        gather.relay(*piece)
    gather.arrive(bits - 1)
    gather.finish()


def errors_kernel(reps, bits, *refs):
    primal_ref, tangent_ref, targets_ref, error_ref, error_tangent_ref = refs[:5]
    refs = refs[5:]
    width = targets_ref.shape[2] // SPLIT
    spans = [(part, pl.ds(i * width, width)) for part in range(2) for i in range(SPLIT)]
    parts = [(primal_ref, tangent_ref)[part].at[:, :, span] for part, span in spans]
    outs = [(error_ref, error_tangent_ref)[part].at[:, :, :, span] for part, span in spans]
    chunks = range(len(spans))
    landing = [refs[c * bits : (c + 1) * bits] for c in chunks]
    refs = refs[len(spans) * bits :]
    totals = [refs[c * bits : (c + 1) * bits] for c in chunks]
    refs = refs[len(spans) * bits :]
    send, recv, local = refs[:3]
    sems = [refs[3 + 6 * c : 9 + 6 * c] for c in chunks]

    place = Place(reps, bits)
    place.meet()
    copies = {}

    def begin(c, j, src):
        half = 1 << (bits - 1 - j)
        copies[c, j] = pltpu.make_async_remote_copy(
            src_ref=src.at[pl.ds((1 - place.bit[j]) * half, half)],
            dst_ref=landing[c][j],
            send_sem=send.at[c, j],
            recv_sem=recv.at[c, j],
            device_id={"fsdp": place.partner[j]},
            device_id_type=MESH,
        )
        copies[c, j].start()

    current = list(parts)
    for c in chunks:
        begin(c, 0, current[c])
    gathers = [Gather(place, outs[c], *sems[c]) for c in chunks]
    own = []
    for j in range(bits):
        half = 1 << (bits - 1 - j)
        for c in chunks:
            copies[c, j].wait_recv()
            keep = place.bit[j] * half
            source, came, total = current[c], landing[c][j], totals[c][j]
            if j < bits - 1:

                def add(i, carry, source=source, came=came, total=total, keep=keep):
                    total[i] = (source[keep + i].astype(F32) + came[i].astype(F32)).astype(BF16)
                    return carry

                lax.fori_loop(0, half, add, 0)
                current[c] = total
                begin(c, j + 1, total)
            else:
                whole = source[keep].astype(F32) + came[0].astype(F32)
                if spans[c][0] == 0:
                    whole = whole - targets_ref[0, :, spans[c][1]].astype(F32)
                total[0] = whole.astype(BF16)
                gathers[c].start(total)
                own.append(
                    pltpu.make_async_copy(
                        total, outs[c].at[0, pl.ds(place.slot, 1)], local.at[c]
                    )
                )
                own[c].start()
    for c in chunks:
        own[c].wait()
    for k in range(bits - 1):
        for c in chunks:
            gathers[c].forward(k)
    for k, piece in enumerate(gathers[0].pieces()):
        for c in chunks:
            gathers[c].relay(*piece)
    for c in chunks:
        gathers[c].arrive(bits - 1)
        gathers[c].finish()
    for copy in copies.values():
        copy.wait_send()


def vmem(count):
    return [pl.BlockSpec(memory_space=pltpu.VMEM)] * count


def gather_tokens(tokens, reps, bits):
    rows, width = tokens.shape
    fsdp = 1 << bits
    out = pl.pallas_call(
        functools.partial(tokens_kernel, reps, bits),
        out_shape=jax.ShapeDtypeStruct((reps, fsdp, rows, width), BF16),
        in_specs=vmem(1),
        out_specs=vmem(1)[0],
        scratch_shapes=[pltpu.SemaphoreType.DMA] + gather_semaphores(reps, bits),
        compiler_params=pltpu.CompilerParams(
            collective_id=0,
            has_side_effects=True,
            vmem_limit_bytes=(reps * fsdp + 1) * rows * width * 2 + (2 << 20),
        ),
        cost_estimate=pl.CostEstimate(flops=0, bytes_accessed=60_000_000, transcendentals=0),
        name="tokens_gather",
    )(tokens.reshape(1, rows, width))
    return out.reshape(reps * fsdp * rows, width)


def exchange_errors(primal, tangent, targets, reps, bits):
    rows, width = targets.shape
    fsdp = 1 << bits
    dma = pltpu.SemaphoreType.DMA
    halves = [pltpu.VMEM((1 << (bits - 1 - j), rows, width // SPLIT), BF16) for j in range(bits)]
    chunks = 2 * SPLIT
    block = rows * width * 2
    limit = block * (2 * fsdp + 4 * fsdp + 2 * reps * fsdp + 2) + (2 << 20)
    shape = jax.ShapeDtypeStruct((reps, fsdp, rows, width), BF16)
    error, error_tangent = pl.pallas_call(
        functools.partial(errors_kernel, reps, bits),
        out_shape=(shape, shape),
        in_specs=vmem(3),
        out_specs=tuple(vmem(2)),
        scratch_shapes=halves * (2 * chunks)
        + [dma((chunks, bits)), dma((chunks, bits)), dma((chunks,))]
        + gather_semaphores(reps, bits) * chunks,
        compiler_params=pltpu.CompilerParams(
            collective_id=1, has_side_effects=True, vmem_limit_bytes=limit
        ),
        cost_estimate=pl.CostEstimate(flops=0, bytes_accessed=120_000_000, transcendentals=0),
        name="errors_exchange",
    )(
        primal.reshape(fsdp, rows, width),
        tangent.reshape(fsdp, rows, width),
        targets.reshape(1, rows, width),
    )
    total = reps * fsdp * rows
    return error.reshape(total, width), error_tangent.reshape(total, width)


def on_device(
    reps,
    bits,
    tokens,
    targets,
    gate_weight,
    up_weight,
    down_weight,
    gate_direction,
    up_direction,
    down_direction,
):
    gathered = gather_tokens(tokens, reps, bits)
    mine = gathered.shape[0] // reps
    gate = jnp.dot(gathered, gate_weight, preferred_element_type=F32)
    up = jnp.dot(gathered, up_weight, preferred_element_type=F32)
    gate_tangent = jnp.dot(gathered, gate_direction, preferred_element_type=F32)
    up_tangent = jnp.dot(gathered, up_direction, preferred_element_type=F32)
    activation, slope, bend = silu_parts(gate)
    hidden = (activation * up).astype(BF16)
    hidden_tangent = (slope * gate_tangent * up + activation * up_tangent).astype(BF16)
    primal = jnp.dot(hidden[:mine], down_weight, preferred_element_type=F32).astype(BF16)
    tangent = (
        jnp.dot(hidden_tangent[:mine], down_weight, preferred_element_type=F32)
        + jnp.dot(hidden[:mine], down_direction, preferred_element_type=F32)
    ).astype(BF16)
    error, error_tangent = exchange_errors(primal, tangent, targets, reps, bits)
    back = jnp.dot(error, down_weight.T, preferred_element_type=F32)
    back_tangent = jnp.dot(error_tangent, down_weight.T, preferred_element_type=F32) + jnp.dot(
        error, down_direction.T, preferred_element_type=F32
    )
    gate_grad_tangent = (
        back_tangent * up * slope + back * up_tangent * slope + back * up * bend * gate_tangent
    ).astype(BF16)
    up_grad_tangent = (back_tangent * activation + back * slope * gate_tangent).astype(BF16)
    hvp_gate = inner_rows(gathered, gate_grad_tangent)
    hvp_up = inner_rows(gathered, up_grad_tangent)
    hvp_down = inner_rows(
        jnp.concatenate([hidden_tangent, hidden], axis=0),
        jnp.concatenate([error, error_tangent], axis=0),
    )
    return (hvp_gate, hvp_up, hvp_down)


def solution(mesh):
    reps = mesh.shape["rep"]
    bits = mesh.shape["fsdp"].bit_length() - 1
    in_specs = (
        P(("rep", "fsdp"), None),
        P(("rep", "fsdp"), None),
        P(None, "fsdp"),
        P(None, "fsdp"),
        P("fsdp", None),
        P(None, "fsdp"),
        P(None, "fsdp"),
        P("fsdp", None),
    )
    out_specs = (P(None, "fsdp"), P(None, "fsdp"), P("fsdp", None))
    return jax.shard_map(
        functools.partial(on_device, reps, bits),
        mesh=mesh, in_specs=in_specs, out_specs=out_specs, check_vma=False,
    )
```
